32 devices in a mesh: branch: 2 (over x), seq: 16 (over z, y, core).
Axes of the slice: x: 2, y: 2, z: 4, core: 2. Of those that a mesh axis runs over, the one named last changes fastest.
Arguments:
- queries: bfloat16 [8192, 2048], P(('branch', 'seq')), parts along dimension 0, may hold values from -8 to 8
- keys: bfloat16 [8192, 2048], P(('branch', 'seq')), parts along dimension 0, may hold values from -8 to 8
- values: bfloat16 [8192, 2048], P(('branch', 'seq')), parts along dimension 0, may hold values from -6 to 6
- out_grad: bfloat16 [8192, 2048], P(('branch', 'seq')), parts along dimension 0, may hold values from -6 to 6
- segments: int32 [8192], P(('branch', 'seq')), parts along dimension 0, may hold values from 0 to 7, never falling along the last dimension, each value on 1 to 768 neighbouring positions
Outputs:
- attended: bfloat16 [8192, 2048], P(('branch', 'seq')), parts along dimension 0
- query_grad: bfloat16 [8192, 2048], P(('branch', 'seq')), parts along dimension 0
- key_grad: bfloat16 [8192, 2048], P(('branch', 'seq')), parts along dimension 0
- value_grad: bfloat16 [8192, 2048], P(('branch', 'seq')), parts along dimension 0
The draws below stay inside these ranges and needn't reach their ends.
There are 2 independent parts, one for each index of `branch`. The reference program is written for one: setup_inputs(seed, part) draws one part's arguments, and reference() takes and returns one part's arrays. A program takes and returns all parts, laid end to end along the dimension named above; each array names one. Nothing has to cross between parts.
Inputs may be any that keep to these rules, and one draw needn't show every extreme that they name: `segments`: never falling along the sequence; each document has 1 to 768 tokens, and one has exactly 768.
All inputs are finite; a program needn't handle non-finite values.
Results may differ from the reference program's by a relative error of at most 0.017.
Values may be sent and summed in bfloat16 or wider, within the bound.
A program may use at most 128 MiB of HBM per device.

```python
import math
import jax
import jax.numpy as jnp
import numpy as np
from jax import lax

HEADS = 16
HDIM = 128
TOK_DEV = 256
REACH = 3
DOC_MAX = 768
TOKENS = 4096
DOCS = 8


def draw_queries(key, part):
    noise_key = jax.random.fold_in(key, 11)
    noise = jax.random.truncated_normal(noise_key, -6.0, 6.0, (TOKENS, HEADS * HDIM), jnp.float32)
    return noise.astype(jnp.bfloat16)


def draw_keys(key, part):
    noise_key = jax.random.fold_in(key, 13)
    noise = jax.random.truncated_normal(noise_key, -6.0, 6.0, (TOKENS, HEADS * HDIM), jnp.float32)
    return noise.astype(jnp.bfloat16)


def steps_of(rng, extent, cuts, smallest, high):
    def one(dim, blocks):
        heights = jax.random.uniform(jax.random.fold_in(jax.random.fold_in(rng, 6), dim), (blocks,), jnp.float32, smallest / len(cuts), high / len(cuts))
        return jnp.repeat(jnp.exp(heights), extent[dim] // blocks).reshape((-1,) + (1,) * (len(extent) - dim - 1))

    factor_of = one(*cuts[0])
    for cut in cuts[1:]:
        factor_of = factor_of * one(*cut)
    return factor_of


def length_profile(amount, total, most, skew):
    weights = [(1 << 20) // math.isqrt(standing ** skew) + 1 for standing in range(2, amount + 1)]
    rest, holding = total - most - (amount - 1), [1] * (amount - 1)
    while rest > 0:
        candidates = [i for i in range(amount - 1) if holding[i] < most]
        mass, budget = sum([weights[i] for i in candidates]), rest
        for i in candidates:
            addition = min(most - holding[i], max(1, budget * weights[i] // mass), rest)
            holding[i] = holding[i] + addition
            rest = rest - addition
    return np.array([most] + holding)


def ragged_sizes(own_key, count, total, reach, slope):
    if count == 2:
        one = jax.random.randint(own_key, (), max(1, total - reach), min(reach, total - 1) + 1)
        return jnp.stack([one, total - one])
    lengths = jnp.asarray(length_profile(count, total, reach, slope), jnp.int32)
    pairs = (count - 1) // 2
    donor, sink = lengths[1:1 + 2 * pairs:2], lengths[2:2 + 2 * pairs:2]
    margin = jnp.minimum(donor - 1, reach - sink)
    moved = jax.random.randint(jax.random.fold_in(own_key, 1), (pairs,), 0, 1 << 20) % (margin + 1)
    lengths = lengths.at[1:1 + 2 * pairs:2].set(donor - moved).at[2:2 + 2 * pairs:2].set(sink + moved)
    return lengths[jax.random.permutation(jax.random.fold_in(own_key, 2), count)]


def bell_draw(stream_key, dims, deviation, most, shards=(), kind=jnp.bfloat16):
    values = jax.random.normal(stream_key, dims, jnp.float32) * deviation
    if len(shards) > 0:
        values = steps_of(stream_key, dims, shards, -0.22, 0.18) * values
    return jnp.clip(values, min=-most, max=most).astype(kind)


def setup_inputs(seed: int = 0, part: int = 0) -> dict:
    arg_keys = jax.random.split(jax.random.key(seed), 6)
    part_keys = jax.random.split(jax.random.fold_in(arg_keys[5], part), 6)
    return {
        "queries": draw_queries(jax.random.fold_in(jax.random.fold_in(arg_keys[5], part), 71), part),
        "keys": draw_keys(jax.random.fold_in(jax.random.fold_in(arg_keys[5], part), 71), part),
        "values": bell_draw(part_keys[2], (TOKENS, HEADS * HDIM), 1.0, 6.0, ((0, 16),)),
        "out_grad": bell_draw(part_keys[3], (TOKENS, HEADS * HDIM), 1.0, 6.0, ((0, 16),)),
        "segments": jnp.searchsorted(jnp.cumsum(ragged_sizes(part_keys[4], DOCS, TOKENS, DOC_MAX, 1)), jnp.arange(TOKENS), side="right").astype(jnp.int32),
    }


def to_half(tensor):
    return lax.optimization_barrier(tensor.astype(jnp.bfloat16)).astype(jnp.float32)

def reference(queries, keys, values, out_grad, segments):
    inv_root = 1.0 / math.sqrt(HDIM)
    pad_rows = REACH * TOK_DEV
    key_width = (REACH + 1) * TOK_DEV
    feature = HEADS * HDIM
    keys_padded = jnp.concatenate([jnp.zeros((pad_rows, feature), keys.dtype), keys], 0)
    values_padded = jnp.concatenate([jnp.zeros((pad_rows, feature), values.dtype), values], 0)
    seg_padded = jnp.concatenate([jnp.full((pad_rows,), -1, jnp.int32), segments.astype(jnp.int32)], 0)

    def one_block(carry, block_index):
        key_acc, value_acc = carry
        start = (block_index * TOK_DEV).astype(jnp.int32)
        query_block = lax.dynamic_slice_in_dim(queries, start, TOK_DEV, 0).reshape(TOK_DEV, HEADS, HDIM).astype(jnp.float32)
        grad_block = lax.dynamic_slice_in_dim(out_grad, start, TOK_DEV, 0).reshape(TOK_DEV, HEADS, HDIM).astype(jnp.float32)
        key_block = lax.dynamic_slice_in_dim(keys_padded, start, key_width, 0).reshape(key_width, HEADS, HDIM).astype(jnp.float32)
        value_block = lax.dynamic_slice_in_dim(values_padded, start, key_width, 0).reshape(key_width, HEADS, HDIM).astype(jnp.float32)
        query_seg = lax.dynamic_slice_in_dim(segments.astype(jnp.int32), start, TOK_DEV, 0)
        key_seg = lax.dynamic_slice_in_dim(seg_padded, start, key_width, 0)
        query_pos = start + jnp.arange(TOK_DEV, dtype=jnp.int32)
        key_pos = start - pad_rows + jnp.arange(key_width, dtype=jnp.int32)
        visible = (key_pos[None, :] <= query_pos[:, None]) & (key_seg[None, :] == query_seg[:, None])
        scores = jnp.einsum('ihd,jhd->hij', query_block, key_block) * inv_root
        scores = jnp.where(visible[None], scores, -jnp.inf)
        row_peak = lax.optimization_barrier(jnp.max(scores, -1, keepdims=True))
        exponent = jnp.exp(scores - row_peak)
        row_total = lax.optimization_barrier(jnp.sum(exponent, -1, keepdims=True))
        weights = to_half(exponent / row_total)
        attended = jnp.einsum('hij,jhd->ihd', weights, value_block).astype(jnp.bfloat16)
        dprob = jnp.einsum('ihd,jhd->hij', grad_block, value_block)
        row_delta = lax.optimization_barrier(jnp.sum(grad_block * attended.astype(jnp.float32), -1)).T
        dscore = to_half(weights * (dprob - row_delta[:, :, None]) * inv_root)
        query_grad = jnp.einsum('hij,jhd->ihd', dscore, key_block).astype(jnp.bfloat16)
        key_part = jnp.einsum('hij,ihd->jhd', dscore, query_block).reshape(key_width, feature)
        value_part = jnp.einsum('hij,ihd->jhd', weights, grad_block).reshape(key_width, feature)
        key_acc = lax.dynamic_update_slice_in_dim(key_acc, lax.dynamic_slice_in_dim(key_acc, start, key_width, 0) + key_part, start, 0)
        value_acc = lax.dynamic_update_slice_in_dim(value_acc, lax.dynamic_slice_in_dim(value_acc, start, key_width, 0) + value_part, start, 0)
        return ((key_acc, value_acc), (attended.reshape(TOK_DEV, feature), query_grad.reshape(TOK_DEV, feature)))
    zeros_acc = jnp.zeros((pad_rows + TOKENS, feature), jnp.float32)
    (key_acc, value_acc), (attended, query_grad) = lax.scan(one_block, (zeros_acc, zeros_acc), jnp.arange(TOKENS // TOK_DEV, dtype=jnp.int32))
    return (attended.reshape(TOKENS, feature), query_grad.reshape(TOKENS, feature), key_acc[pad_rows:].astype(jnp.bfloat16), value_acc[pad_rows:].astype(jnp.bfloat16))
```

```python
import functools
import math

import jax
import jax.numpy as jnp
from jax import lax
from jax.experimental import pallas as pl
from jax.experimental.pallas import tpu as pltpu
from jax.sharding import PartitionSpec as P

HEADS = 16
REACH = 3
AHEAD = 4
VMEM_LIMIT = 49 * 1024 * 1024
MESH = pl.DeviceIdType.MESH
HIDDEN = -1e30
NT = (((1,), (1,)), ((), ()))
NN = (((1,), (0,)), ((), ()))


def dot(a, b, dims):
    return lax.dot_general(a, b, dims, preferred_element_type=jnp.float32)


def kernel(
    count, rows, head_dim,
    q_in, k_in, v_in, g_in, seg_row, seg_col,
    o_out, dq_out, dk_out, dv_out,
    qb, kb, vb, gb, kseg, qseg, stat, bias, bias_t,
    load_sem, send_sem, recv_sem, seg_send, seg_recv, stat_send, stat_recv,
):
    me = lax.axis_index("seq")
    odd = me % 2
    second = (me // 2) % 2
    partner = me + 1 - 2 * odd
    chunks = HEADS
    pairs = count // 4
    pair = me // 4
    inv_root = 1.0 / math.sqrt(head_dim)
    log2_scale = inv_root * math.log2(math.e)
    bufs = (kb, vb, qb, gb)
    ins = (k_in, v_in, q_in, g_in)
    KV, QG = (0, 1), (2, 3)
    far = range(1, REACH + 1)

    def to(target):
        return {"seq": target}

    def columns(c):
        return pl.ds(pl.multiple_of(c * head_dim, head_dim), head_dim)

    def piece(t, slot, c):
        return bufs[t].at[slot, :, columns(c)]

    def load(t, slot, cols):
        return bufs[t][slot, :, cols]

    def send(ts, from_slot, to_slot, kind, c, target):
        for t in ts:
            pltpu.make_async_remote_copy(
                src_ref=piece(t, from_slot, c),
                dst_ref=piece(t, to_slot, c),
                send_sem=send_sem.at[t, kind, c],
                recv_sem=recv_sem.at[t, to_slot, c],
                device_id=to(target),
                device_id_type=MESH,
            ).start()

    def landed(ts, slot, c):
        for t in ts:
            pltpu.make_async_copy(piece(t, slot, c), piece(t, slot, c), recv_sem.at[t, slot, c]).wait()

    direct_up = me + 1 + 2 * odd
    direct_down = me - 3 + 2 * odd
    slot_up = 1 + 2 * odd
    slot_down = 3 - 2 * odd
    first = second == 0
    last = second == 1
    below = pair >= 1
    above = pair + 1 < pairs

    def share(c, amount):
        return (c + 1) * amount // chunks > c * amount // chunks

    def kv_near(row, c):
        return share(c, chunks * (pairs - 1 - row) // pairs)

    def qg_near(row, c):
        return share(c, chunks * row // pairs)

    def active(ts, kind, c):
        if ts == KV:
            return (
                first & (me + 2 < count),
                direct_up < count,
                me - 2 >= 0,
                last & (odd == 0) & above & jnp.logical_not(kv_near(pair, c)),
                last & below & jnp.logical_not(kv_near(pair - 1, c)),
                last & above & kv_near(pair, c),
                first & above & kv_near(pair, c),
            )[kind]
        return (
            last & (me - 2 >= 0),
            direct_down >= 0,
            me + 2 < count,
            first & (odd == 1) & below & jnp.logical_not(qg_near(pair, c)),
            first & above & jnp.logical_not(qg_near(pair + 1, c)),
            first & below & qg_near(pair, c),
            last & below & qg_near(pair, c),
        )[kind]

    loads = [pltpu.make_async_copy(ins[t], bufs[t].at[0], load_sem.at[t]) for t in range(4)]
    for copy in loads:
        copy.start()

    barrier = pltpu.get_barrier_semaphore()
    met = 0
    for d in (1, 2, 3, 4, 5):
        for peer, there in ((me + d, me + d < count), (me - d, me - d >= 0)):
            @pl.when(there)
            def _():
                pl.semaphore_signal(barrier, inc=1, device_id=to(peer), device_id_type=MESH)
            met = met + jnp.where(there, 1, 0)
    pl.semaphore_wait(barrier, met)

    def seg_copy(way, d, target):
        return pltpu.make_async_remote_copy(
            src_ref=seg_row,
            dst_ref=(kseg, qseg)[way].at[d],
            send_sem=seg_send.at[way, d],
            recv_sem=seg_recv.at[way, d],
            device_id=to(target),
            device_id_type=MESH,
        )

    def direct(ts, c):
        slot, target = (slot_up, direct_up) if ts == KV else (slot_down, direct_down)

        @pl.when(active(ts, 1, c))
        def _():
            send(ts, 0, slot, 1, c, target)

        @pl.when(active(ts, 3, c))
        def _():
            send(ts, 0, 4, 3, c, me + 5 if ts == KV else me - 5)

    def own_y(ts, c):
        @pl.when(active(ts, 0, c))
        def _():
            send(ts, 0, 2, 0, c, me + 2 if ts == KV else me - 2)

    def near_start(ts, c):
        @pl.when(active(ts, 5, c))
        def _():
            send(ts, 0, 4, 5, c, me - 2 if ts == KV else me + 2)

    def near_end(ts, c):
        @pl.when(active(ts, 6, c))
        def _():
            landed(ts, 4, c)
            send(ts, 4, 2, 6, c, me + 4 if ts == KV else me - 4)

    def far_end(ts, c):
        slot, target = (3 + odd, me - 1 - 2 * odd) if ts == KV else (4 - odd, me + 3 - 2 * odd)

        @pl.when(active(ts, 4, c))
        def _():
            landed(ts, slot, c)
            send(ts, slot, 2, 4, c, target)

    def relay(ts, c):
        @pl.when(active(ts, 2, c))
        def _():
            landed(ts, 2, c)
            send(ts, 2, slot_down if ts == KV else slot_up, 2, c, partner)

    for d in far:
        @pl.when(me + d < count)
        def _():
            seg_copy(0, d, me + d).start()

        @pl.when(me - d >= 0)
        def _():
            seg_copy(1, d, me - d).start()

    def start_keys(c, carry):
        own_y(KV, c)

        @pl.when(c < AHEAD)
        def _():
            near_start(KV, c)

        direct(KV, c)
        return carry

    def start_queries(c, carry):
        direct(QG, c)
        return carry

    for copy in loads[:2]:
        copy.wait()
    lax.fori_loop(0, chunks, start_keys, 0)
    for copy in loads[2:]:
        copy.wait()
    lax.fori_loop(0, chunks, start_queries, 0)

    for d in far:
        @pl.when(me - d < 0)
        def _():
            kb[d] = jnp.zeros(kb.shape[1:], kb.dtype)
            vb[d] = jnp.zeros(vb.shape[1:], vb.dtype)
            kseg[d] = jnp.full(kseg.shape[1:], -1, kseg.dtype)

        @pl.when(me + d >= count)
        def _():
            qb[d] = jnp.zeros(qb.shape[1:], qb.dtype)
            gb[d] = jnp.zeros(gb.shape[1:], gb.dtype)
            qseg[d] = jnp.full(qseg.shape[1:], -1, qseg.dtype)
            stat[d] = jnp.zeros(stat.shape[1:], stat.dtype)

    far_end(KV, 0)
    own_col = jnp.broadcast_to(seg_col[...], (rows, rows))
    upper = lax.broadcasted_iota(jnp.int32, (rows, rows), 0)
    across = lax.broadcasted_iota(jnp.int32, (rows, rows), 1)
    same = own_col == seg_row[0:1, :]
    bias[0] = jnp.where(same & (across <= upper), 0.0, HIDDEN)
    bias_t[0] = jnp.where(same & (upper <= across), 0.0, HIDDEN)
    for d in far:
        @pl.when(me - d >= 0)
        def _():
            pltpu.make_async_copy(seg_row, kseg.at[d], seg_recv.at[0, d]).wait()

        @pl.when(me + d < count)
        def _():
            pltpu.make_async_copy(seg_row, qseg.at[d], seg_recv.at[1, d]).wait()
        bias[d] = jnp.where(own_col == kseg[d, 0:1, :], 0.0, HIDDEN)
        bias_t[d] = jnp.where(own_col == qseg[d, 0:1, :], 0.0, HIDDEN)
    near_end(KV, 0)
    relay(KV, 0)

    first_lane = lax.broadcasted_iota(jnp.int32, (rows, head_dim), 1) == 0
    span = range(REACH + 1)

    def own_queries(c):
        cols = columns(c)
        query = load(2, 0, cols)
        grad = load(3, 0, cols)
        scores = [dot(query, load(0, d, cols), NT) * log2_scale + bias[d] for d in span]
        peak = jnp.max(functools.reduce(jnp.maximum, scores), -1, keepdims=True)
        exponent = [jnp.exp2(s - peak) for s in scores]
        total = jnp.sum(functools.reduce(jnp.add, exponent), -1, keepdims=True)
        inverse = 1.0 / total
        weights = [(e * inverse).astype(jnp.bfloat16) for e in exponent]
        attended = functools.reduce(
            jnp.add, [dot(weights[d], load(1, d, cols), NN) for d in span]
        ).astype(jnp.bfloat16)
        o_out[:, cols] = attended
        delta = jnp.sum(grad.astype(jnp.float32) * attended.astype(jnp.float32), -1, keepdims=True)
        pair = jnp.where(first_lane, peak + jnp.log2(total), delta)
        stat[0, c] = pair.T[0:2]
        total_grad = None
        for d in span:
            dprob = dot(grad, load(1, d, cols), NT)
            dscore = (weights[d].astype(jnp.float32) * (dprob - delta)).astype(jnp.bfloat16)
            term = dot(dscore, load(0, d, cols), NN)
            total_grad = term if total_grad is None else total_grad + term
        dq_out[:, cols] = (total_grad * inv_root).astype(jnp.bfloat16)

    def own_keys(c):
        cols = columns(c)
        key = load(0, 0, cols)
        value = load(1, 0, cols)
        key_grad = value_grad = None
        for d in span:
            query = load(2, d, cols)
            grad = load(3, d, cols)
            lse = stat[d, c, 0:1, :]
            delta = stat[d, c, 1:2, :]
            scores = dot(key, query, NT) * log2_scale + bias_t[d]
            weights = jnp.exp2(scores - lse)
            dprob = dot(value, grad, NT)
            dscore = (weights * (dprob - delta)).astype(jnp.bfloat16)
            value_term = dot(weights.astype(jnp.bfloat16), grad, NN)
            key_term = dot(dscore, query, NN)
            value_grad = value_term if value_grad is None else value_grad + value_term
            key_grad = key_term if key_grad is None else key_grad + key_term
        dk_out[:, cols] = (key_grad * inv_root).astype(jnp.bfloat16)
        dv_out[:, cols] = value_grad.astype(jnp.bfloat16)

    def send_stats(c):
        for d in far:
            @pl.when(me - d >= 0)
            def _():
                pltpu.make_async_remote_copy(
                    src_ref=stat.at[0, c],
                    dst_ref=stat.at[d, c],
                    send_sem=stat_send.at[d, c],
                    recv_sem=stat_recv.at[d, c],
                    device_id=to(me - d),
                    device_id_type=MESH,
                ).start()

    def arrive_queries(c):
        @pl.when(me - 1 >= 0)
        def _():
            landed(KV, 1, c)

        @pl.when((me - 3 >= 0) & jnp.logical_not((odd == 0) & active(KV, 4, c)))
        def _():
            landed(KV, 3, c)

    def arrive_keys(c):
        @pl.when(me + 1 < count)
        def _():
            landed(QG, 1, c)

        @pl.when((me + 3 < count) & jnp.logical_not((odd == 1) & active(QG, 4, c)))
        def _():
            landed(QG, 3, c)
        for d in far:
            @pl.when(me + d < count)
            def _():
                pltpu.make_async_copy(stat.at[d, c], stat.at[d, c], stat_recv.at[d, c]).wait()

    def query_step(c, carry):
        @pl.when(c + AHEAD < chunks)
        def _():
            near_start(KV, c + AHEAD)

        @pl.when(c + 1 < chunks)
        def _():
            far_end(KV, c + 1)
            near_end(KV, c + 1)
            relay(KV, c + 1)

        near_start(QG, c)
        far_end(QG, c)

        @pl.when(c % pairs == 0)
        def _():
            own_y(QG, c // pairs)

        arrive_queries(c)
        own_queries(c)
        send_stats(c)
        return carry

    def key_step(c, carry):
        @pl.when(c + 1 < chunks)
        def _():
            near_end(QG, c + 1)
            relay(QG, c + 1)

        arrive_keys(c)
        own_keys(c)
        return carry

    def own_rest(c, carry):
        own_y(QG, c)
        return carry

    lax.fori_loop(0, chunks, query_step, 0)
    lax.fori_loop(-(-chunks // pairs), chunks, own_rest, 0)
    near_end(QG, 0)
    relay(QG, 0)
    lax.fori_loop(0, chunks, key_step, 0)

    def finish(c, carry):
        for ts in (KV, QG):
            for kind in range(7):
                @pl.when(active(ts, kind, c))
                def _():
                    for t in ts:
                        pltpu.make_async_copy(piece(t, 0, c), piece(t, 0, c), send_sem.at[t, kind, c]).wait()
        for d in far:
            @pl.when(me - d >= 0)
            def _():
                pltpu.make_async_copy(stat.at[0, c], stat.at[0, c], stat_send.at[d, c]).wait()
        return carry

    lax.fori_loop(0, chunks, finish, 0)
    for d in far:
        @pl.when(me + d < count)
        def _():
            pltpu.make_async_copy(seg_row, seg_row, seg_send.at[0, d]).wait()

        @pl.when(me - d >= 0)
        def _():
            pltpu.make_async_copy(seg_row, seg_row, seg_send.at[1, d]).wait()


def solution(mesh):
    count = mesh.shape["seq"]

    def local(queries, keys, values, out_grad, segments):
        rows, feature = queries.shape
        head_dim = feature // HEADS
        seg_row = jnp.broadcast_to(segments[None, :], (8, rows))
        seg_col = segments[:, None]
        vmem = pl.BlockSpec(memory_space=pltpu.VMEM)
        slots = REACH + 1
        block = pltpu.VMEM((slots + 1, rows, feature), queries.dtype)
        seg_block = pltpu.VMEM((slots, 8, rows), jnp.int32)
        mask = pltpu.VMEM((slots, rows, rows), jnp.float32)
        dma = pltpu.SemaphoreType.DMA
        return pl.pallas_call(
            functools.partial(kernel, count, rows, head_dim),
            out_shape=[jax.ShapeDtypeStruct((rows, feature), jnp.bfloat16)] * 4,
            in_specs=[pl.BlockSpec(memory_space=pl.ANY)] * 4 + [vmem] * 2,
            out_specs=[vmem] * 4,
            scratch_shapes=[block] * 4 + [
                seg_block, seg_block,
                pltpu.VMEM((slots, HEADS, 2, rows), jnp.float32),
                mask, mask,
                dma((4,)), dma((4, 7, HEADS)), dma((4, slots + 1, HEADS)),
                dma((2, slots)), dma((2, slots)), dma((slots, HEADS)), dma((slots, HEADS)),
            ],
            compiler_params=pltpu.CompilerParams(
                collective_id=0, has_side_effects=True, vmem_limit_bytes=VMEM_LIMIT
            ),
        )(queries, keys, values, out_grad, seg_row, seg_col)

    rows_spec = P(("branch", "seq"), None)
    return jax.shard_map(
        local,
        mesh=mesh,
        in_specs=(rows_spec,) * 4 + (P(("branch", "seq")),),
        out_specs=(rows_spec,) * 4,
        check_vma=False,
    )
```

```python
import functools
import math

import jax
import jax.numpy as jnp
from jax import lax
from jax.experimental import pallas as pl
from jax.experimental.pallas import tpu as pltpu
from jax.sharding import PartitionSpec as P

HEADS = 16
REACH = 3
FILL = 6
VMEM_LIMIT = 49 * 1024 * 1024
MESH = pl.DeviceIdType.MESH
HIDDEN = -1e30
NT = (((1,), (1,)), ((), ()))
NN = (((1,), (0,)), ((), ()))


def dot(a, b, dims):
    return lax.dot_general(a, b, dims, preferred_element_type=jnp.float32)


def kernel(
    count, rows, head_dim,
    q_in, k_in, v_in, g_in, seg_row, seg_col,
    o_out, dq_out, dk_out, dv_out,
    qb, kb, vb, gb, kseg, qseg, stat, bias, bias_t,
    load_sem, send_sem, recv_sem, seg_send, seg_recv, stat_send, stat_recv,
):
    me = lax.axis_index("seq")
    odd = me % 2
    second = (me // 2) % 2
    partner = me + 1 - 2 * odd
    chunks = HEADS
    pairs = count // 4
    pair = me // 4
    inv_root = 1.0 / math.sqrt(head_dim)
    log2_scale = inv_root * math.log2(math.e)
    bufs = (kb, vb, qb, gb)
    ins = (k_in, v_in, q_in, g_in)
    KV, QG = (0, 1), (2, 3)
    far = range(1, REACH + 1)

    def to(target):
        return {"seq": target}

    def columns(c):
        return pl.ds(pl.multiple_of(c * head_dim, head_dim), head_dim)

    def piece(t, slot, c):
        return bufs[t].at[slot, :, columns(c)]

    def load(t, slot, cols):
        return bufs[t][slot, :, cols]

    def send(ts, from_slot, to_slot, kind, c, target):
        for t in ts:
            pltpu.make_async_remote_copy(
                src_ref=piece(t, from_slot, c),
                dst_ref=piece(t, to_slot, c),
                send_sem=send_sem.at[t, kind, c],
                recv_sem=recv_sem.at[t, to_slot, c],
                device_id=to(target),
                device_id_type=MESH,
            ).start()

    def landed(ts, slot, c):
        for t in ts:
            pltpu.make_async_copy(piece(t, slot, c), piece(t, slot, c), recv_sem.at[t, slot, c]).wait()

    direct_up = me + 1 + 2 * odd
    direct_down = me - 3 + 2 * odd
    slot_up = 1 + 2 * odd
    slot_down = 3 - 2 * odd
    first = second == 0
    last = second == 1
    below = pair >= 1
    above = pair + 1 < pairs

    def kv_near(row, c):
        return c < chunks * (pairs - 1 - row) // pairs - 1

    def qg_near(row, c):
        return c < (chunks - chunks // pairs) * row // pairs

    paced = first & (odd == 1) & above & kv_near(pair, 0)

    def active(ts, kind, c):
        if ts == KV:
            return (
                first & (me + 2 < count),
                direct_up < count,
                me - 2 >= 0,
                last & (odd == 0) & above & jnp.logical_not(kv_near(pair, c)),
                last & below & jnp.logical_not(kv_near(pair - 1, c)),
                last & above & kv_near(pair, c),
                first & above & kv_near(pair, c),
            )[kind]
        return (
            last & (me - 2 >= 0),
            direct_down >= 0,
            me + 2 < count,
            first & (odd == 1) & below & jnp.logical_not(qg_near(pair, c)),
            first & above & jnp.logical_not(qg_near(pair + 1, c)),
            first & below & qg_near(pair, c),
            last & below & qg_near(pair, c),
        )[kind]

    loads = [pltpu.make_async_copy(ins[t], bufs[t].at[0], load_sem.at[t]) for t in range(4)]
    for copy in loads:
        copy.start()

    barrier = pltpu.get_barrier_semaphore()
    met = 0
    for d in (1, 2, 3, 4, 5):
        for peer, there in ((me + d, me + d < count), (me - d, me - d >= 0)):
            @pl.when(there)
            def _():
                pl.semaphore_signal(barrier, inc=1, device_id=to(peer), device_id_type=MESH)
            met = met + jnp.where(there, 1, 0)
    pl.semaphore_wait(barrier, met)

    def seg_copy(way, d, target):
        return pltpu.make_async_remote_copy(
            src_ref=seg_row,
            dst_ref=(kseg, qseg)[way].at[d],
            send_sem=seg_send.at[way, d],
            recv_sem=seg_recv.at[way, d],
            device_id=to(target),
            device_id_type=MESH,
        )

    def direct(ts, c):
        slot, target = (slot_up, direct_up) if ts == KV else (slot_down, direct_down)

        @pl.when(active(ts, 1, c))
        def _():
            send(ts, 0, slot, 1, c, target)

        @pl.when(active(ts, 3, c))
        def _():
            send(ts, 0, 4, 3, c, me + 5 if ts == KV else me - 5)

    def own_y(ts, c):
        @pl.when(active(ts, 0, c))
        def _():
            send(ts, 0, 2, 0, c, me + 2 if ts == KV else me - 2)

    def near_start(ts, c):
        @pl.when(active(ts, 5, c))
        def _():
            send(ts, 0, 4, 5, c, me - 2 if ts == KV else me + 2)

    def near_end(ts, c):
        @pl.when(active(ts, 6, c))
        def _():
            landed(ts, 4, c)
            send(ts, 4, 2, 6, c, me + 4 if ts == KV else me - 4)

    def far_end(ts, c):
        slot, target = (3 + odd, me - 1 - 2 * odd) if ts == KV else (4 - odd, me + 3 - 2 * odd)

        @pl.when(active(ts, 4, c))
        def _():
            landed(ts, slot, c)
            send(ts, slot, 2, 4, c, target)

    def relay(ts, c):
        @pl.when(active(ts, 2, c))
        def _():
            landed(ts, 2, c)
            send(ts, 2, slot_down if ts == KV else slot_up, 2, c, partner)

    for d in far:
        @pl.when(me + d < count)
        def _():
            seg_copy(0, d, me + d).start()

        @pl.when(me - d >= 0)
        def _():
            seg_copy(1, d, me - d).start()

    def start_keys(c, carry):
        own_y(KV, c)
        near_start(KV, c)

        @pl.when(jnp.logical_not(paced) | (c == 0))
        def _():
            direct(KV, c)
        return carry

    def start_queries(c, carry):
        @pl.when(c < FILL)
        def _():
            own_y(QG, c)

        direct(QG, c)
        near_start(QG, c)
        return carry

    def direct_rest(c, carry):
        direct(KV, c)
        return carry

    def step_y(c):
        far_end(KV, c)
        near_end(KV, c)

        @pl.when(paced)
        def _():
            stop = jnp.where(kv_near(pair, c + 1), c + 2, chunks)
            lax.fori_loop(c + 1, jnp.where(kv_near(pair, c), stop, c + 1), direct_rest, 0)

        relay(KV, c)

    for copy in loads[:2]:
        copy.wait()
    lax.fori_loop(0, chunks, start_keys, 0)
    for copy in loads[2:]:
        copy.wait()
    lax.fori_loop(0, chunks, start_queries, 0)

    for d in far:
        @pl.when(me - d < 0)
        def _():
            kb[d] = jnp.zeros(kb.shape[1:], kb.dtype)
            vb[d] = jnp.zeros(vb.shape[1:], vb.dtype)
            kseg[d] = jnp.full(kseg.shape[1:], -1, kseg.dtype)

        @pl.when(me + d >= count)
        def _():
            qb[d] = jnp.zeros(qb.shape[1:], qb.dtype)
            gb[d] = jnp.zeros(gb.shape[1:], gb.dtype)
            qseg[d] = jnp.full(qseg.shape[1:], -1, qseg.dtype)
            stat[d] = jnp.zeros(stat.shape[1:], stat.dtype)

    own_col = jnp.broadcast_to(seg_col[...], (rows, rows))
    upper = lax.broadcasted_iota(jnp.int32, (rows, rows), 0)
    across = lax.broadcasted_iota(jnp.int32, (rows, rows), 1)
    same = own_col == seg_row[0:1, :]
    bias[0] = jnp.where(same & (across <= upper), 0.0, HIDDEN)
    bias_t[0] = jnp.where(same & (upper <= across), 0.0, HIDDEN)
    for d in far:
        @pl.when(me - d >= 0)
        def _():
            pltpu.make_async_copy(seg_row, kseg.at[d], seg_recv.at[0, d]).wait()

        @pl.when(me + d < count)
        def _():
            pltpu.make_async_copy(seg_row, qseg.at[d], seg_recv.at[1, d]).wait()
        bias[d] = jnp.where(own_col == kseg[d, 0:1, :], 0.0, HIDDEN)
        bias_t[d] = jnp.where(own_col == qseg[d, 0:1, :], 0.0, HIDDEN)
    step_y(0)

    first_lane = lax.broadcasted_iota(jnp.int32, (rows, head_dim), 1) == 0
    span = range(REACH + 1)

    def own_queries(c):
        cols = columns(c)
        query = load(2, 0, cols)
        grad = load(3, 0, cols)
        scores = [dot(query, load(0, d, cols), NT) * log2_scale + bias[d] for d in span]
        peak = jnp.max(functools.reduce(jnp.maximum, scores), -1, keepdims=True)
        exponent = [jnp.exp2(s - peak) for s in scores]
        total = jnp.sum(functools.reduce(jnp.add, exponent), -1, keepdims=True)
        inverse = 1.0 / total
        weights = [(e * inverse).astype(jnp.bfloat16) for e in exponent]
        attended = functools.reduce(
            jnp.add, [dot(weights[d], load(1, d, cols), NN) for d in span]
        ).astype(jnp.bfloat16)
        o_out[:, cols] = attended
        delta = jnp.sum(grad.astype(jnp.float32) * attended.astype(jnp.float32), -1, keepdims=True)
        pair = jnp.where(first_lane, peak + jnp.log2(total), delta)
        stat[0, c] = pair.T[0:2]
        total_grad = None
        for d in span:
            dprob = dot(grad, load(1, d, cols), NT)
            dscore = (weights[d].astype(jnp.float32) * (dprob - delta)).astype(jnp.bfloat16)
            term = dot(dscore, load(0, d, cols), NN)
            total_grad = term if total_grad is None else total_grad + term
        dq_out[:, cols] = (total_grad * inv_root).astype(jnp.bfloat16)

    def own_keys(c):
        cols = columns(c)
        key = load(0, 0, cols)
        value = load(1, 0, cols)
        key_grad = value_grad = None
        for d in span:
            query = load(2, d, cols)
            grad = load(3, d, cols)
            lse = stat[d, c, 0:1, :]
            delta = stat[d, c, 1:2, :]
            scores = dot(key, query, NT) * log2_scale + bias_t[d]
            weights = jnp.exp2(scores - lse)
            dprob = dot(value, grad, NT)
            dscore = (weights * (dprob - delta)).astype(jnp.bfloat16)
            value_term = dot(weights.astype(jnp.bfloat16), grad, NN)
            key_term = dot(dscore, query, NN)
            value_grad = value_term if value_grad is None else value_grad + value_term
            key_grad = key_term if key_grad is None else key_grad + key_term
        dk_out[:, cols] = (key_grad * inv_root).astype(jnp.bfloat16)
        dv_out[:, cols] = value_grad.astype(jnp.bfloat16)

    def send_stats(c):
        for d in far:
            @pl.when(me - d >= 0)
            def _():
                pltpu.make_async_remote_copy(
                    src_ref=stat.at[0, c],
                    dst_ref=stat.at[d, c],
                    send_sem=stat_send.at[d, c],
                    recv_sem=stat_recv.at[d, c],
                    device_id=to(me - d),
                    device_id_type=MESH,
                ).start()

    def arrive_queries(c):
        @pl.when(me - 1 >= 0)
        def _():
            landed(KV, 1, c)

        @pl.when((me - 3 >= 0) & jnp.logical_not((odd == 0) & active(KV, 4, c)))
        def _():
            landed(KV, 3, c)

    def arrive_keys(c):
        @pl.when(me + 1 < count)
        def _():
            landed(QG, 1, c)

        @pl.when((me + 3 < count) & jnp.logical_not((odd == 1) & active(QG, 4, c)))
        def _():
            landed(QG, 3, c)
        for d in far:
            @pl.when(me + d < count)
            def _():
                pltpu.make_async_copy(stat.at[d, c], stat.at[d, c], stat_recv.at[d, c]).wait()

    def own_rest(c, carry):
        own_y(QG, c)
        return carry

    def query_step(c, carry):
        @pl.when(c + 1 < chunks)
        def _():
            step_y(c + 1)

        far_end(QG, c)

        @pl.when(c + 2 == chunks)
        def _():
            lax.fori_loop(FILL, chunks, own_rest, 0)

        arrive_queries(c)
        own_queries(c)
        send_stats(c)
        return carry

    def key_step(c, carry):
        @pl.when(c + 1 < chunks)
        def _():
            near_end(QG, c + 1)
            relay(QG, c + 1)

        arrive_keys(c)
        own_keys(c)
        return carry

    lax.fori_loop(0, chunks, query_step, 0)
    near_end(QG, 0)
    relay(QG, 0)
    lax.fori_loop(0, chunks, key_step, 0)

    def finish(c, carry):
        for ts in (KV, QG):
            for kind in range(7):
                @pl.when(active(ts, kind, c))
                def _():
                    for t in ts:
                        pltpu.make_async_copy(piece(t, 0, c), piece(t, 0, c), send_sem.at[t, kind, c]).wait()
        for d in far:
            @pl.when(me - d >= 0)
            def _():
                pltpu.make_async_copy(stat.at[0, c], stat.at[0, c], stat_send.at[d, c]).wait()
        return carry

    lax.fori_loop(0, chunks, finish, 0)
    for d in far:
        @pl.when(me + d < count)
        def _():
            pltpu.make_async_copy(seg_row, seg_row, seg_send.at[0, d]).wait()

        @pl.when(me - d >= 0)
        def _():
            pltpu.make_async_copy(seg_row, seg_row, seg_send.at[1, d]).wait()


def solution(mesh):
    count = mesh.shape["seq"]

    def local(queries, keys, values, out_grad, segments):
        rows, feature = queries.shape
        head_dim = feature // HEADS
        seg_row = jnp.broadcast_to(segments[None, :], (8, rows))
        seg_col = segments[:, None]
        vmem = pl.BlockSpec(memory_space=pltpu.VMEM)
        slots = REACH + 1
        block = pltpu.VMEM((slots + 1, rows, feature), queries.dtype)
        seg_block = pltpu.VMEM((slots, 8, rows), jnp.int32)
        mask = pltpu.VMEM((slots, rows, rows), jnp.float32)
        dma = pltpu.SemaphoreType.DMA
        return pl.pallas_call(
            functools.partial(kernel, count, rows, head_dim),
            out_shape=[jax.ShapeDtypeStruct((rows, feature), jnp.bfloat16)] * 4,
            in_specs=[pl.BlockSpec(memory_space=pl.ANY)] * 4 + [vmem] * 2,
            out_specs=[vmem] * 4,
            scratch_shapes=[block] * 4 + [
                seg_block, seg_block,
                pltpu.VMEM((slots, HEADS, 2, rows), jnp.float32),
                mask, mask,
                dma((4,)), dma((4, 7, HEADS)), dma((4, slots + 1, HEADS)),
                dma((2, slots)), dma((2, slots)), dma((slots, HEADS)), dma((slots, HEADS)),
            ],
            compiler_params=pltpu.CompilerParams(
                collective_id=0, has_side_effects=True, vmem_limit_bytes=VMEM_LIMIT
            ),
        )(queries, keys, values, out_grad, seg_row, seg_col)

    rows_spec = P(("branch", "seq"), None)
    return jax.shard_map(
        local,
        mesh=mesh,
        in_specs=(rows_spec,) * 4 + (P(("branch", "seq")),),
        out_specs=(rows_spec,) * 4,
        check_vma=False,
    )
```

```python
import functools
import math

import jax
import jax.numpy as jnp
from jax import lax
from jax.experimental import pallas as pl
from jax.experimental.pallas import tpu as pltpu
from jax.sharding import PartitionSpec as P

HEADS = 16
REACH = 3
FILL = 6
LAG = 4
DRAIN_LIMIT = 48 * 1024 * 1024
VMEM_LIMIT = 49 * 1024 * 1024
MESH = pl.DeviceIdType.MESH
HIDDEN = -1e30
NT = (((1,), (1,)), ((), ()))
NN = (((1,), (0,)), ((), ()))


def dot(a, b, dims):
    return lax.dot_general(a, b, dims, preferred_element_type=jnp.float32)


def kernel(
    count, rows, head_dim,
    q_in, k_in, v_in, g_in, seg_in,
    o_out, dq_out, dk_out, dv_out,
    kvb, qgb, seg_row, kseg, qseg, stat, bias, bias_t,
    load_sem, send_sem, recv_sem, seg_send, seg_recv, stat_send, stat_recv,
):
    me = lax.axis_index("seq")
    odd = me % 2
    second = (me // 2) % 2
    partner = me + 1 - 2 * odd
    chunks = HEADS
    pairs = count // 4
    pair = me // 4
    inv_root = 1.0 / math.sqrt(head_dim)
    log2_scale = inv_root * math.log2(math.e)
    bufs = (kvb, qgb)
    ins = (k_in, v_in, q_in, g_in)
    KV, QG = 0, 1
    far = range(1, REACH + 1)

    def to(target):
        return {"seq": target}

    def columns(c):
        return pl.ds(pl.multiple_of(c * head_dim, head_dim), head_dim)

    def piece(ts, slot, c):
        return bufs[ts].at[slot, :, :, columns(c)]

    def load(t, slot, cols):
        return bufs[t // 2][slot, t % 2, :, cols]

    def send(ts, from_slot, to_slot, kind, c, target):
        pltpu.make_async_remote_copy(
            src_ref=piece(ts, from_slot, c),
            dst_ref=piece(ts, to_slot, c),
            send_sem=send_sem.at[ts, kind, c],
            recv_sem=recv_sem.at[ts, to_slot, c],
            device_id=to(target),
            device_id_type=MESH,
        ).start()

    def landed(ts, slot, c):
        pltpu.make_async_copy(piece(ts, slot, c), piece(ts, slot, c), recv_sem.at[ts, slot, c]).wait()

    direct_up = me + 1 + 2 * odd
    direct_down = me - 3 + 2 * odd
    slot_up = 1 + 2 * odd
    slot_down = 3 - 2 * odd
    first = second == 0
    last = second == 1
    below = pair >= 1
    above = pair + 1 < pairs

    def kv_near(row, c):
        return c < chunks * (pairs - 1 - row) // pairs - 1

    def qg_near(row, c):
        return c < (chunks - chunks // pairs) * row // pairs

    paced = first & (odd == 1) & above & kv_near(pair, 0)

    def active(ts, kind, c):
        if ts == KV:
            return (
                first & (me + 2 < count),
                direct_up < count,
                me - 2 >= 0,
                last & (odd == 0) & above & jnp.logical_not(kv_near(pair, c)),
                last & below & jnp.logical_not(kv_near(pair - 1, c)),
                last & above & kv_near(pair, c),
                first & above & kv_near(pair, c),
            )[kind]
        return (
            last & (me - 2 >= 0),
            direct_down >= 0,
            me + 2 < count,
            first & (odd == 1) & below & jnp.logical_not(qg_near(pair, c)),
            first & above & jnp.logical_not(qg_near(pair + 1, c)),
            first & below & qg_near(pair, c),
            last & below & qg_near(pair, c),
        )[kind]

    loads = [pltpu.make_async_copy(ins[t], bufs[t // 2].at[0, t % 2], load_sem.at[t]) for t in range(4)]
    loads.append(pltpu.make_async_copy(seg_in, seg_row, load_sem.at[4]))
    for copy in loads:
        copy.start()

    barrier = pltpu.get_barrier_semaphore()
    met = 0
    for d in (1, 2, 3, 4, 5):
        for peer, there in ((me + d, me + d < count), (me - d, me - d >= 0)):
            @pl.when(there)
            def _():
                pl.semaphore_signal(barrier, inc=1, device_id=to(peer), device_id_type=MESH)
            met = met + jnp.where(there, 1, 0)
    pl.semaphore_wait(barrier, met)

    def seg_copy(way, d, target):
        return pltpu.make_async_remote_copy(
            src_ref=seg_row,
            dst_ref=(kseg, qseg)[way].at[d],
            send_sem=seg_send.at[way, d],
            recv_sem=seg_recv.at[way, d],
            device_id=to(target),
            device_id_type=MESH,
        )

    def direct(ts, c):
        slot, target = (slot_up, direct_up) if ts == KV else (slot_down, direct_down)

        @pl.when(active(ts, 1, c))
        def _():
            send(ts, 0, slot, 1, c, target)

        @pl.when(active(ts, 3, c))
        def _():
            send(ts, 0, 4, 3, c, me + 5 if ts == KV else me - 5)

    def own_y(ts, c):
        @pl.when(active(ts, 0, c))
        def _():
            send(ts, 0, 2, 0, c, me + 2 if ts == KV else me - 2)

    def near_start(ts, c):
        @pl.when(active(ts, 5, c))
        def _():
            send(ts, 0, 4, 5, c, me - 2 if ts == KV else me + 2)

    def near_end(ts, c):
        @pl.when(active(ts, 6, c))
        def _():
            landed(ts, 4, c)
            send(ts, 4, 2, 6, c, me + 4 if ts == KV else me - 4)

    def far_end(ts, c):
        slot, target = (3 + odd, me - 1 - 2 * odd) if ts == KV else (4 - odd, me + 3 - 2 * odd)

        @pl.when(active(ts, 4, c))
        def _():
            landed(ts, slot, c)
            send(ts, slot, 2, 4, c, target)

    def relay(ts, c):
        @pl.when(active(ts, 2, c))
        def _():
            landed(ts, 2, c)
            send(ts, 2, slot_down if ts == KV else slot_up, 2, c, partner)

    loads[4].wait()
    for d in far:
        @pl.when(me + d < count)
        def _():
            seg_copy(0, d, me + d).start()

        @pl.when(me - d >= 0)
        def _():
            seg_copy(1, d, me - d).start()

    def start_keys(c, carry):
        own_y(KV, c)
        near_start(KV, c)

        @pl.when(jnp.logical_not(paced) | (c == 0))
        def _():
            direct(KV, c)
        return carry

    def start_queries(c, carry):
        @pl.when(c < FILL)
        def _():
            own_y(QG, c)

        direct(QG, c)
        near_start(QG, c)
        return carry

    def direct_rest(c, carry):
        direct(KV, c)
        return carry

    def step_y(c):
        far_end(KV, c)
        near_end(KV, c)

        @pl.when(paced)
        def _():
            stop = jnp.where(kv_near(pair, c + 1), c + 2, chunks)
            lax.fori_loop(c + 1, jnp.where(kv_near(pair, c), stop, c + 1), direct_rest, 0)

        relay(KV, c)

    for copy in loads[:2]:
        copy.wait()
    lax.fori_loop(0, chunks, start_keys, 0)
    for copy in loads[2:4]:
        copy.wait()
    lax.fori_loop(0, chunks, start_queries, 0)

    for d in far:
        @pl.when(me - d < 0)
        def _():
            kvb[d] = jnp.zeros(kvb.shape[1:], kvb.dtype)
            kseg[d] = jnp.full(kseg.shape[1:], -1, kseg.dtype)

        @pl.when(me + d >= count)
        def _():
            qgb[d] = jnp.zeros(qgb.shape[1:], qgb.dtype)
            qseg[d] = jnp.full(qseg.shape[1:], -1, qseg.dtype)
            stat[d] = jnp.zeros(stat.shape[1:], stat.dtype)

    own_col = jnp.broadcast_to(seg_row[0:1, :], (rows, rows)).T
    upper = lax.broadcasted_iota(jnp.int32, (rows, rows), 0)
    across = lax.broadcasted_iota(jnp.int32, (rows, rows), 1)
    same = own_col == seg_row[0:1, :]
    bias[0] = jnp.where(same & (across <= upper), 0.0, HIDDEN)
    bias_t[0] = jnp.where(same & (upper <= across), 0.0, HIDDEN)
    for d in far:
        @pl.when(me - d >= 0)
        def _():
            pltpu.make_async_copy(seg_row, kseg.at[d], seg_recv.at[0, d]).wait()

        @pl.when(me + d < count)
        def _():
            pltpu.make_async_copy(seg_row, qseg.at[d], seg_recv.at[1, d]).wait()
        bias[d] = jnp.where(own_col == kseg[d, 0:1, :], 0.0, HIDDEN)
        bias_t[d] = jnp.where(own_col == qseg[d, 0:1, :], 0.0, HIDDEN)
    step_y(0)

    first_lane = lax.broadcasted_iota(jnp.int32, (rows, head_dim), 1) == 0
    span = range(REACH + 1)

    def own_queries(c):
        cols = columns(c)
        query = load(2, 0, cols)
        grad = load(3, 0, cols)
        scores = [dot(query, load(0, d, cols), NT) * log2_scale + bias[d] for d in span]
        peak = jnp.max(functools.reduce(jnp.maximum, scores), -1, keepdims=True)
        exponent = [jnp.exp2(s - peak) for s in scores]
        total = jnp.sum(functools.reduce(jnp.add, exponent), -1, keepdims=True)
        inverse = 1.0 / total
        weights = [(e * inverse).astype(jnp.bfloat16) for e in exponent]
        attended = functools.reduce(
            jnp.add, [dot(weights[d], load(1, d, cols), NN) for d in span]
        ).astype(jnp.bfloat16)
        o_out[:, cols] = attended
        delta = jnp.sum(grad.astype(jnp.float32) * attended.astype(jnp.float32), -1, keepdims=True)
        pair = jnp.where(first_lane, peak + jnp.log2(total), delta)
        stat[0, c] = pair.T[0:2]
        total_grad = None
        for d in span:
            dprob = dot(grad, load(1, d, cols), NT)
            dscore = (weights[d].astype(jnp.float32) * (dprob - delta)).astype(jnp.bfloat16)
            term = dot(dscore, load(0, d, cols), NN)
            total_grad = term if total_grad is None else total_grad + term
        dq_out[:, cols] = (total_grad * inv_root).astype(jnp.bfloat16)

    def own_keys(c):
        cols = columns(c)
        key = load(0, 0, cols)
        value = load(1, 0, cols)
        key_grad = value_grad = None
        for d in span:
            query = load(2, d, cols)
            grad = load(3, d, cols)
            lse = stat[d, c, 0:1, :]
            delta = stat[d, c, 1:2, :]
            scores = dot(key, query, NT) * log2_scale + bias_t[d]
            weights = jnp.exp2(scores - lse)
            dprob = dot(value, grad, NT)
            dscore = (weights * (dprob - delta)).astype(jnp.bfloat16)
            value_term = dot(weights.astype(jnp.bfloat16), grad, NN)
            key_term = dot(dscore, query, NN)
            value_grad = value_term if value_grad is None else value_grad + value_term
            key_grad = key_term if key_grad is None else key_grad + key_term
        dk_out[:, cols] = (key_grad * inv_root).astype(jnp.bfloat16)
        dv_out[:, cols] = value_grad.astype(jnp.bfloat16)

    def send_stats(c):
        for d in far:
            @pl.when(me - d >= 0)
            def _():
                pltpu.make_async_remote_copy(
                    src_ref=stat.at[0, c],
                    dst_ref=stat.at[d, c],
                    send_sem=stat_send.at[d, c],
                    recv_sem=stat_recv.at[d, c],
                    device_id=to(me - d),
                    device_id_type=MESH,
                ).start()

    def arrive_queries(c):
        @pl.when(me - 1 >= 0)
        def _():
            landed(KV, 1, c)

        @pl.when((me - 3 >= 0) & jnp.logical_not((odd == 0) & active(KV, 4, c)))
        def _():
            landed(KV, 3, c)

    def arrive_keys(c):
        @pl.when(me + 1 < count)
        def _():
            landed(QG, 1, c)

        @pl.when((me + 3 < count) & jnp.logical_not((odd == 1) & active(QG, 4, c)))
        def _():
            landed(QG, 3, c)
        for d in far:
            @pl.when(me + d < count)
            def _():
                pltpu.make_async_copy(stat.at[d, c], stat.at[d, c], stat_recv.at[d, c]).wait()

    def own_rest(c, carry):
        own_y(QG, c)
        return carry

    def query_step(c, carry):
        @pl.when(c + 1 < chunks)
        def _():
            step_y(c + 1)

        far_end(QG, c)

        @pl.when(c + 2 == chunks)
        def _():
            lax.fori_loop(FILL, chunks, own_rest, 0)

        arrive_queries(c)
        own_queries(c)
        send_stats(c)
        return carry

    def sent(ts, c):
        for kind in range(7):
            @pl.when(active(ts, kind, c))
            def _():
                pltpu.make_async_copy(piece(ts, 0, c), piece(ts, 0, c), send_sem.at[ts, kind, c]).wait()

    def finish(c):
        sent(KV, c)
        sent(QG, c)
        for d in far:
            @pl.when(me - d >= 0)
            def _():
                pltpu.make_async_copy(stat.at[0, c], stat.at[0, c], stat_send.at[d, c]).wait()

    def finish_rest(c, carry):
        finish(c)
        return carry

    def key_step(c, carry):
        @pl.when(c + 1 < chunks)
        def _():
            near_end(QG, c + 1)
            relay(QG, c + 1)

        @pl.when(c >= LAG)
        def _():
            finish(c - LAG)

        arrive_keys(c)
        own_keys(c)
        return carry

    lax.fori_loop(0, chunks, query_step, 0)
    near_end(QG, 0)
    relay(QG, 0)
    lax.fori_loop(0, chunks, key_step, 0)

    lax.fori_loop(chunks - LAG, chunks, finish_rest, 0)
    for d in far:
        @pl.when(me + d < count)
        def _():
            pltpu.make_async_copy(seg_row, seg_row, seg_send.at[0, d]).wait()

        @pl.when(me - d >= 0)
        def _():
            pltpu.make_async_copy(seg_row, seg_row, seg_send.at[1, d]).wait()


def drain(*refs):
    ins, outs, sem = refs[:4], refs[4:8], refs[8]
    copies = [pltpu.make_async_copy(ins[t], outs[t], sem.at[t]) for t in range(4)]
    for copy in copies:
        copy.start()
    for copy in copies:
        copy.wait()


def solution(mesh):
    count = mesh.shape["seq"]

    def local(queries, keys, values, out_grad, segments):
        rows, feature = queries.shape
        head_dim = feature // HEADS
        vmem = pl.BlockSpec(memory_space=pltpu.VMEM)
        slots = REACH + 1
        block = pltpu.VMEM((slots + 1, 2, rows, feature), queries.dtype)
        seg_block = pltpu.VMEM((slots, 1, rows), jnp.int32)
        mask = pltpu.VMEM((slots, rows, rows), jnp.float32)
        dma = pltpu.SemaphoreType.DMA
        shapes = [jax.ShapeDtypeStruct((rows, feature), jnp.bfloat16)] * 4
        results = pl.pallas_call(
            functools.partial(kernel, count, rows, head_dim),
            out_shape=shapes,
            in_specs=[pl.BlockSpec(memory_space=pl.ANY)] * 5,
            out_specs=[vmem] * 4,
            scratch_shapes=[block] * 2 + [
                pltpu.VMEM((1, rows), jnp.int32), seg_block, seg_block,
                pltpu.VMEM((slots, HEADS, 2, rows), jnp.float32),
                mask, mask,
                dma((5,)), dma((2, 7, HEADS)), dma((2, slots + 1, HEADS)),
                dma((2, slots)), dma((2, slots)), dma((slots, HEADS)), dma((slots, HEADS)),
            ],
            compiler_params=pltpu.CompilerParams(
                collective_id=0, has_side_effects=True, vmem_limit_bytes=VMEM_LIMIT
            ),
        )(queries, keys, values, out_grad, segments[None, :])
        return pl.pallas_call(
            drain,
            out_shape=shapes,
            in_specs=[vmem] * 4,
            out_specs=[pl.BlockSpec(memory_space=pl.ANY)] * 4,
            scratch_shapes=[dma((4,))],
            compiler_params=pltpu.CompilerParams(vmem_limit_bytes=DRAIN_LIMIT),
        )(*results)

    rows_spec = P(("branch", "seq"), None)
    return jax.shard_map(
        local,
        mesh=mesh,
        in_specs=(rows_spec,) * 4 + (P(("branch", "seq")),),
        out_specs=(rows_spec,) * 4,
        check_vma=False,
    )
```

```python
import functools
import math

import jax
import jax.numpy as jnp
from jax import lax
from jax.experimental import pallas as pl
from jax.experimental.pallas import tpu as pltpu
from jax.sharding import PartitionSpec as P

HEADS = 16
REACH = 3
FILL = 6
LAG = 4
DRAIN_LIMIT = 48 * 1024 * 1024
VMEM_LIMIT = 49 * 1024 * 1024
MESH = pl.DeviceIdType.MESH
HIDDEN = -1e30
NT = (((1,), (1,)), ((), ()))
NN = (((1,), (0,)), ((), ()))


def dot(a, b, dims):
    return lax.dot_general(a, b, dims, preferred_element_type=jnp.float32)


def kernel(
    count, rows, head_dim,
    q_in, k_in, v_in, g_in, seg_in,
    o_out, dq_out, dk_out, dv_out,
    kvb, qgb, seg_row, kseg, qseg, stat, bias, bias_t,
    load_sem, whole_sem, send_sem, recv_sem, seg_send, seg_recv, stat_send, stat_recv,
):
    me = lax.axis_index("seq")
    odd = me % 2
    second = (me // 2) % 2
    partner = me + 1 - 2 * odd
    chunks = HEADS
    pairs = count // 4
    pair = me // 4
    inv_root = 1.0 / math.sqrt(head_dim)
    log2_scale = inv_root * math.log2(math.e)
    bufs = (kvb, qgb)
    ins = (k_in, v_in, q_in, g_in)
    KV, QG = 0, 1
    far = range(1, REACH + 1)

    def to(target):
        return {"seq": target}

    def columns(c):
        return pl.ds(pl.multiple_of(c * head_dim, head_dim), head_dim)

    def piece(ts, slot, c):
        return bufs[ts].at[slot, :, :, columns(c)]

    def load(t, slot, cols):
        return bufs[t // 2][slot, t % 2, :, cols]

    def send(ts, from_slot, to_slot, kind, c, target):
        pltpu.make_async_remote_copy(
            src_ref=piece(ts, from_slot, c),
            dst_ref=piece(ts, to_slot, c),
            send_sem=whole_sem.at[ts, kind] if kind < 3 else send_sem.at[ts, c],
            recv_sem=recv_sem.at[ts, to_slot - 1, c],
            device_id=to(target),
            device_id_type=MESH,
        ).start()

    def landed(ts, slot, c):
        pltpu.make_async_copy(piece(ts, slot, c), piece(ts, slot, c), recv_sem.at[ts, slot - 1, c]).wait()

    def wait_many(part, sem, there):
        for n in far:
            @pl.when(there == n if n < REACH else there >= n)
            def _():
                pltpu.make_async_copy(part(n), part(n), sem).wait()

    direct_up = me + 1 + 2 * odd
    direct_down = me - 3 + 2 * odd
    slot_up = 1 + 2 * odd
    slot_down = 3 - 2 * odd
    first = second == 0
    last = second == 1
    below = pair >= 1
    above = pair + 1 < pairs

    def kv_near(row, c):
        return c < chunks * (pairs - 1 - row) // pairs

    def qg_near(row, c):
        return c < (chunks - chunks // pairs) * row // pairs

    paced = first & (odd == 1) & above & kv_near(pair, 0)

    def active(ts, kind, c):
        if ts == KV:
            return (
                first & (me + 2 < count),
                direct_up < count,
                me - 2 >= 0,
                last & (odd == 0) & above & jnp.logical_not(kv_near(pair, c)),
                last & below & jnp.logical_not(kv_near(pair - 1, c)),
                last & above & kv_near(pair, c),
                first & above & kv_near(pair, c),
            )[kind]
        return (
            last & (me - 2 >= 0),
            direct_down >= 0,
            me + 2 < count,
            first & (odd == 1) & below & jnp.logical_not(qg_near(pair, c)),
            first & above & jnp.logical_not(qg_near(pair + 1, c)),
            first & below & qg_near(pair, c),
            last & below & qg_near(pair, c),
        )[kind]

    loads = [pltpu.make_async_copy(ins[t], bufs[t // 2].at[0, t % 2], load_sem.at[t]) for t in range(4)]
    loads.append(pltpu.make_async_copy(seg_in, seg_row, load_sem.at[4]))
    for copy in loads:
        copy.start()

    barrier = pltpu.get_barrier_semaphore()
    met = 0
    for d in (1, 2, 3, 4, 5):
        for peer, there in (
            (me + d, (me + d < count) & ((d < 5) | (odd == 0))),
            (me - d, (me - d >= 0) & ((d < 5) | (odd == 1))),
        ):
            @pl.when(there)
            def _():
                pl.semaphore_signal(barrier, inc=1, device_id=to(peer), device_id_type=MESH)
            met = met + jnp.where(there, 1, 0)
    pl.semaphore_wait(barrier, met)

    def seg_copy(way, d, target):
        return pltpu.make_async_remote_copy(
            src_ref=seg_row,
            dst_ref=(kseg, qseg)[way].at[d],
            send_sem=seg_send.at[way],
            recv_sem=seg_recv.at[way],
            device_id=to(target),
            device_id_type=MESH,
        )

    def direct(ts, c):
        slot, target = (slot_up, direct_up) if ts == KV else (slot_down, direct_down)

        @pl.when(active(ts, 1, c))
        def _():
            send(ts, 0, slot, 1, c, target)

        @pl.when(active(ts, 3, c))
        def _():
            send(ts, 0, 4, 3, c, me + 5 if ts == KV else me - 5)

    def own_y(ts, c):
        @pl.when(active(ts, 0, c))
        def _():
            send(ts, 0, 2, 0, c, me + 2 if ts == KV else me - 2)

    def near_start(ts, c):
        @pl.when(active(ts, 5, c))
        def _():
            send(ts, 0, 4, 5, c, me - 2 if ts == KV else me + 2)

    def near_end(ts, c):
        @pl.when(active(ts, 6, c))
        def _():
            landed(ts, 4, c)
            send(ts, 4, 2, 6, c, me + 4 if ts == KV else me - 4)

    def far_end(ts, c):
        slot, target = (3 + odd, me - 1 - 2 * odd) if ts == KV else (4 - odd, me + 3 - 2 * odd)

        @pl.when(active(ts, 4, c))
        def _():
            landed(ts, slot, c)
            send(ts, slot, 2, 4, c, target)

    def relay(ts, c):
        @pl.when(active(ts, 2, c))
        def _():
            landed(ts, 2, c)
            send(ts, 2, slot_down if ts == KV else slot_up, 2, c, partner)

    loads[4].wait()
    for d in far:
        @pl.when(me + d < count)
        def _():
            seg_copy(0, d, me + d).start()

        @pl.when(me - d >= 0)
        def _():
            seg_copy(1, d, me - d).start()

    def start_keys(c, carry):
        own_y(KV, c)
        near_start(KV, c)

        @pl.when(jnp.logical_not(paced) | (c == 0))
        def _():
            direct(KV, c)
        return carry

    def start_queries(c, carry):
        @pl.when(c < FILL)
        def _():
            own_y(QG, c)

        direct(QG, c)
        near_start(QG, c)
        return carry

    def direct_rest(c, carry):
        direct(KV, c)
        return carry

    def step_y(c):
        far_end(KV, c)
        near_end(KV, c)

        @pl.when(paced)
        def _():
            stop = jnp.where(kv_near(pair, c + 1), c + 2, chunks)
            lax.fori_loop(c + 1, jnp.where(kv_near(pair, c), stop, c + 1), direct_rest, 0)

        relay(KV, c)

    for copy in loads[:2]:
        copy.wait()
    lax.fori_loop(0, chunks, start_keys, 0)
    for copy in loads[2:4]:
        copy.wait()
    lax.fori_loop(0, chunks, start_queries, 0)

    for d in far:
        @pl.when(me - d < 0)
        def _():
            kvb[d] = jnp.zeros(kvb.shape[1:], kvb.dtype)
            kseg[d] = jnp.full(kseg.shape[1:], -1, kseg.dtype)

        @pl.when(me + d >= count)
        def _():
            qgb[d] = jnp.zeros(qgb.shape[1:], qgb.dtype)
            qseg[d] = jnp.full(qseg.shape[1:], -1, qseg.dtype)
            stat[d] = jnp.zeros(stat.shape[1:], stat.dtype)

    own_col = jnp.broadcast_to(seg_row[0:1, :], (rows, rows)).T
    upper = lax.broadcasted_iota(jnp.int32, (rows, rows), 0)
    across = lax.broadcasted_iota(jnp.int32, (rows, rows), 1)
    same = own_col == seg_row[0:1, :]
    bias[0] = jnp.where(same & (across <= upper), 0.0, HIDDEN)
    bias_t[0] = jnp.where(same & (upper <= across), 0.0, HIDDEN)
    wait_many(lambda n: kseg.at[pl.ds(1, n)], seg_recv.at[0], me)
    wait_many(lambda n: qseg.at[pl.ds(1, n)], seg_recv.at[1], count - 1 - me)
    for d in far:
        bias[d] = jnp.where(own_col == kseg[d, 0:1, :], 0.0, HIDDEN)
        bias_t[d] = jnp.where(own_col == qseg[d, 0:1, :], 0.0, HIDDEN)
    step_y(0)

    first_lane = lax.broadcasted_iota(jnp.int32, (rows, head_dim), 1) == 0
    span = range(REACH + 1)

    def own_queries(c):
        cols = columns(c)
        query = load(2, 0, cols)
        grad = load(3, 0, cols)
        scores = [dot(query, load(0, d, cols), NT) * log2_scale + bias[d] for d in span]
        peak = jnp.max(functools.reduce(jnp.maximum, scores), -1, keepdims=True)
        exponent = [jnp.exp2(s - peak) for s in scores]
        total = jnp.sum(functools.reduce(jnp.add, exponent), -1, keepdims=True)
        inverse = 1.0 / total
        weights = [(e * inverse).astype(jnp.bfloat16) for e in exponent]
        attended = functools.reduce(
            jnp.add, [dot(weights[d], load(1, d, cols), NN) for d in span]
        ).astype(jnp.bfloat16)
        o_out[:, cols] = attended
        delta = jnp.sum(grad.astype(jnp.float32) * attended.astype(jnp.float32), -1, keepdims=True)
        pair = jnp.where(first_lane, peak + jnp.log2(total), delta)
        stat[0, c] = pair.T[0:2]
        total_grad = None
        for d in span:
            dprob = dot(grad, load(1, d, cols), NT)
            dscore = (weights[d].astype(jnp.float32) * (dprob - delta)).astype(jnp.bfloat16)
            term = dot(dscore, load(0, d, cols), NN)
            total_grad = term if total_grad is None else total_grad + term
        dq_out[:, cols] = (total_grad * inv_root).astype(jnp.bfloat16)

    def own_keys(c):
        cols = columns(c)
        key = load(0, 0, cols)
        value = load(1, 0, cols)
        key_grad = value_grad = None
        for d in span:
            query = load(2, d, cols)
            grad = load(3, d, cols)
            lse = stat[d, c, 0:1, :]
            delta = stat[d, c, 1:2, :]
            scores = dot(key, query, NT) * log2_scale + bias_t[d]
            weights = jnp.exp2(scores - lse)
            dprob = dot(value, grad, NT)
            dscore = (weights * (dprob - delta)).astype(jnp.bfloat16)
            value_term = dot(weights.astype(jnp.bfloat16), grad, NN)
            key_term = dot(dscore, query, NN)
            value_grad = value_term if value_grad is None else value_grad + value_term
            key_grad = key_term if key_grad is None else key_grad + key_term
        dk_out[:, cols] = (key_grad * inv_root).astype(jnp.bfloat16)
        dv_out[:, cols] = value_grad.astype(jnp.bfloat16)

    def send_stats(c):
        for d in far:
            @pl.when(me - d >= 0)
            def _():
                pltpu.make_async_remote_copy(
                    src_ref=stat.at[0, c],
                    dst_ref=stat.at[d, c],
                    send_sem=stat_send.at[d - 1],
                    recv_sem=stat_recv.at[c],
                    device_id=to(me - d),
                    device_id_type=MESH,
                ).start()

    def arrive_queries(c):
        @pl.when(me - 1 >= 0)
        def _():
            landed(KV, 1, c)

        @pl.when((me - 3 >= 0) & jnp.logical_not((odd == 0) & active(KV, 4, c)))
        def _():
            landed(KV, 3, c)

    def arrive_keys(c):
        @pl.when(me + 1 < count)
        def _():
            landed(QG, 1, c)

        @pl.when((me + 3 < count) & jnp.logical_not((odd == 1) & active(QG, 4, c)))
        def _():
            landed(QG, 3, c)
        wait_many(lambda n: stat.at[pl.ds(1, n), c], stat_recv.at[c], count - 1 - me)

    def own_rest(c, carry):
        own_y(QG, c)
        return carry

    def query_step(c, carry):
        @pl.when(c + 1 < chunks)
        def _():
            step_y(c + 1)

        far_end(QG, c)

        @pl.when(c + 2 == chunks)
        def _():
            lax.fori_loop(FILL, chunks, own_rest, 0)

        arrive_queries(c)
        own_queries(c)
        send_stats(c)
        return carry

    def finish(c):
        for ts in (KV, QG):
            own = active(ts, 3, c) | active(ts, 5, c) | active(ts, 6, c)
            passed = active(ts, 4, c)
            for slots, there in ((2, own & passed), (1, own != passed)):
                @pl.when(there)
                def _():
                    part = bufs[ts].at[pl.ds(0, slots), :, :, columns(c)]
                    pltpu.make_async_copy(part, part, send_sem.at[ts, c]).wait()

    def finish_rest(c, carry):
        finish(c)
        return carry

    def key_step(c, carry):
        @pl.when(c + 1 < chunks)
        def _():
            near_end(QG, c + 1)
            relay(QG, c + 1)

        @pl.when(c >= LAG)
        def _():
            finish(c - LAG)

        arrive_keys(c)
        own_keys(c)
        return carry

    lax.fori_loop(0, chunks, query_step, 0)
    near_end(QG, 0)
    relay(QG, 0)
    lax.fori_loop(0, chunks, key_step, 0)

    lax.fori_loop(chunks - LAG, chunks, finish_rest, 0)
    for ts in (KV, QG):
        for kind in range(3):
            @pl.when(active(ts, kind, 0))
            def _():
                pltpu.make_async_copy(bufs[ts].at[0], bufs[ts].at[0], whole_sem.at[ts, kind]).wait()
    for d in far:
        @pl.when(me - d >= 0)
        def _():
            pltpu.make_async_copy(stat.at[0], stat.at[0], stat_send.at[d - 1]).wait()

    wait_many(lambda n: kseg.at[pl.ds(1, n)], seg_send.at[0], count - 1 - me)
    wait_many(lambda n: kseg.at[pl.ds(1, n)], seg_send.at[1], me)


def drain(*refs):
    ins, outs, sem = refs[:4], refs[4:8], refs[8]
    copies = [pltpu.make_async_copy(ins[t], outs[t], sem.at[t]) for t in range(4)]
    for copy in copies:
        copy.start()
    for copy in copies:
        copy.wait()


def solution(mesh):
    count = mesh.shape["seq"]

    def local(queries, keys, values, out_grad, segments):
        rows, feature = queries.shape
        head_dim = feature // HEADS
        vmem = pl.BlockSpec(memory_space=pltpu.VMEM)
        slots = REACH + 1
        block = pltpu.VMEM((slots + 1, 2, rows, feature), queries.dtype)
        seg_block = pltpu.VMEM((slots, 1, rows), jnp.int32)
        mask = pltpu.VMEM((slots, rows, rows), jnp.float32)
        dma = pltpu.SemaphoreType.DMA
        shapes = [jax.ShapeDtypeStruct((rows, feature), jnp.bfloat16)] * 4
        results = pl.pallas_call(
            functools.partial(kernel, count, rows, head_dim),
            out_shape=shapes,
            in_specs=[pl.BlockSpec(memory_space=pl.ANY)] * 5,
            out_specs=[vmem] * 4,
            scratch_shapes=[block] * 2 + [
                pltpu.VMEM((1, rows), jnp.int32), seg_block, seg_block,
                pltpu.VMEM((slots, HEADS, 2, rows), jnp.float32),
                mask, mask,
                dma((5,)), dma((2, 3)), dma((2, HEADS)), dma((2, slots, HEADS)),
                dma((2,)), dma((2,)), dma((REACH,)), dma((HEADS,)),
            ],
            compiler_params=pltpu.CompilerParams(
                collective_id=0, has_side_effects=True, vmem_limit_bytes=VMEM_LIMIT
            ),
        )(queries, keys, values, out_grad, segments[None, :])
        return pl.pallas_call(
            drain,
            out_shape=shapes,
            in_specs=[vmem] * 4,
            out_specs=[pl.BlockSpec(memory_space=pl.ANY)] * 4,
            scratch_shapes=[dma((4,))],
            compiler_params=pltpu.CompilerParams(vmem_limit_bytes=DRAIN_LIMIT),
        )(*results)

    rows_spec = P(("branch", "seq"), None)
    return jax.shard_map(
        local,
        mesh=mesh,
        in_specs=(rows_spec,) * 4 + (P(("branch", "seq")),),
        out_specs=(rows_spec,) * 4,
        check_vma=False,
    )
```

```python
import functools
import math

import jax
import jax.numpy as jnp
from jax import lax
from jax.experimental import pallas as pl
from jax.experimental.pallas import tpu as pltpu
from jax.sharding import PartitionSpec as P

HEADS = 16
REACH = 3
FILL = 6
LAG = 2
DRAIN_LIMIT = 48 * 1024 * 1024
VMEM_LIMIT = 49 * 1024 * 1024
MESH = pl.DeviceIdType.MESH
HIDDEN = -1e30
NT = (((1,), (1,)), ((), ()))
NN = (((1,), (0,)), ((), ()))


def dot(a, b, dims):
    return lax.dot_general(a, b, dims, preferred_element_type=jnp.float32)


def kernel(
    count, rows, head_dim,
    q_in, k_in, v_in, g_in, seg_in,
    o_out, dq_out, dk_out, dv_out,
    kvb, qgb, seg_row, kseg, qseg, stat, bias, bias_t,
    load_sem, whole_sem, send_sem, recv_sem, seg_send, seg_recv, stat_send, stat_recv,
):
    me = lax.axis_index("seq")
    odd = me % 2
    second = (me // 2) % 2
    partner = me + 1 - 2 * odd
    chunks = HEADS
    pairs = count // 4
    pair = me // 4
    inv_root = 1.0 / math.sqrt(head_dim)
    log2_scale = inv_root * math.log2(math.e)
    bufs = (kvb, qgb)
    ins = (k_in, v_in, q_in, g_in)
    KV, QG = 0, 1
    far = range(1, REACH + 1)

    def to(target):
        return {"seq": target}

    def columns(c):
        return pl.ds(pl.multiple_of(c * head_dim, head_dim), head_dim)

    def piece(ts, slot, c):
        return bufs[ts].at[slot, :, :, columns(c)]

    def load(t, slot, cols):
        return bufs[t // 2][slot, t % 2, :, cols]

    def send(ts, from_slot, to_slot, kind, c, target):
        pltpu.make_async_remote_copy(
            src_ref=piece(ts, from_slot, c),
            dst_ref=piece(ts, to_slot, c),
            send_sem=whole_sem.at[ts, kind] if kind < 3 else send_sem.at[ts, c],
            recv_sem=recv_sem.at[ts, to_slot - 1, c],
            device_id=to(target),
            device_id_type=MESH,
        ).start()

    def landed(ts, slot, c):
        pltpu.make_async_copy(piece(ts, slot, c), piece(ts, slot, c), recv_sem.at[ts, slot - 1, c]).wait()

    def wait_many(part, sem, there):
        for n in far:
            @pl.when(there == n if n < REACH else there >= n)
            def _():
                pltpu.make_async_copy(part(n), part(n), sem).wait()

    direct_up = me + 1 + 2 * odd
    direct_down = me - 3 + 2 * odd
    slot_up = 1 + 2 * odd
    slot_down = 3 - 2 * odd
    first = second == 0
    last = second == 1
    below = pair >= 1
    above = pair + 1 < pairs

    def kv_near(row, c):
        return c < chunks * (pairs - 1 - row) // pairs

    def qg_near(row, c, parity):
        amount = (chunks - chunks // pairs) * row // pairs
        early = chunks * 3 // 8
        late = ((c - early) % 2 == 1) & (c < 2 * amount - early)
        return (c < jnp.minimum(amount, early)) | ((c >= early) & late)

    paced = first & (odd == 1) & above & kv_near(pair, 0)

    def active(ts, kind, c):
        if ts == KV:
            return (
                first & (me + 2 < count),
                direct_up < count,
                me - 2 >= 0,
                last & (odd == 0) & above & jnp.logical_not(kv_near(pair, c)),
                last & below & jnp.logical_not(kv_near(pair - 1, c)),
                last & above & kv_near(pair, c),
                first & above & kv_near(pair, c),
            )[kind]
        return (
            last & (me - 2 >= 0),
            direct_down >= 0,
            me + 2 < count,
            first & (odd == 1) & below & jnp.logical_not(qg_near(pair, c, odd)),
            first & above & jnp.logical_not(qg_near(pair + 1, c, 1 - odd)),
            first & below & qg_near(pair, c, odd),
            last & below & qg_near(pair, c, odd),
        )[kind]

    loads = [pltpu.make_async_copy(ins[t], bufs[t // 2].at[0, t % 2], load_sem.at[t]) for t in range(4)]
    loads.append(pltpu.make_async_copy(seg_in, seg_row, load_sem.at[4]))
    for copy in loads:
        copy.start()

    barrier = pltpu.get_barrier_semaphore()
    met = 0
    for d in (1, 2, 3, 4, 5):
        for peer, there in (
            (me + d, (me + d < count) & ((d < 5) | (odd == 0))),
            (me - d, (me - d >= 0) & ((d < 5) | (odd == 1))),
        ):
            @pl.when(there)
            def _():
                pl.semaphore_signal(barrier, inc=1, device_id=to(peer), device_id_type=MESH)
            met = met + jnp.where(there, 1, 0)
    pl.semaphore_wait(barrier, met)

    def seg_copy(way, d, target):
        return pltpu.make_async_remote_copy(
            src_ref=seg_row,
            dst_ref=(kseg, qseg)[way].at[d],
            send_sem=seg_send.at[way],
            recv_sem=seg_recv.at[way],
            device_id=to(target),
            device_id_type=MESH,
        )

    def direct(ts, c):
        slot, target = (slot_up, direct_up) if ts == KV else (slot_down, direct_down)

        @pl.when(active(ts, 1, c))
        def _():
            send(ts, 0, slot, 1, c, target)

        @pl.when(active(ts, 3, c))
        def _():
            send(ts, 0, 4, 3, c, me + 5 if ts == KV else me - 5)

    def own_y(ts, c):
        @pl.when(active(ts, 0, c))
        def _():
            send(ts, 0, 2, 0, c, me + 2 if ts == KV else me - 2)

    def near_start(ts, c):
        @pl.when(active(ts, 5, c))
        def _():
            send(ts, 0, 4, 5, c, me - 2 if ts == KV else me + 2)

    def near_end(ts, c):
        @pl.when(active(ts, 6, c))
        def _():
            landed(ts, 4, c)
            send(ts, 4, 2, 6, c, me + 4 if ts == KV else me - 4)

    def far_end(ts, c):
        slot, target = (3 + odd, me - 1 - 2 * odd) if ts == KV else (4 - odd, me + 3 - 2 * odd)

        @pl.when(active(ts, 4, c))
        def _():
            landed(ts, slot, c)
            send(ts, slot, 2, 4, c, target)

    def relay(ts, c):
        @pl.when(active(ts, 2, c))
        def _():
            landed(ts, 2, c)
            send(ts, 2, slot_down if ts == KV else slot_up, 2, c, partner)

    loads[4].wait()
    for d in far:
        @pl.when(me + d < count)
        def _():
            seg_copy(0, d, me + d).start()

        @pl.when(me - d >= 0)
        def _():
            seg_copy(1, d, me - d).start()

    def start_keys(c, carry):
        own_y(KV, c)
        near_start(KV, c)

        @pl.when(jnp.logical_not(paced) | (c == 0))
        def _():
            direct(KV, c)
        return carry

    def start_queries(c, carry):
        @pl.when(c < FILL)
        def _():
            own_y(QG, c)

        direct(QG, c)
        near_start(QG, c)
        return carry

    def direct_rest(c, carry):
        direct(KV, c)
        return carry

    def step_y(c):
        far_end(KV, c)
        near_end(KV, c)

        @pl.when(paced)
        def _():
            stop = jnp.where(kv_near(pair, c + 1), c + 2, chunks)
            lax.fori_loop(c + 1, jnp.where(kv_near(pair, c), stop, c + 1), direct_rest, 0)

        relay(KV, c)

    for copy in loads[:2]:
        copy.wait()
    lax.fori_loop(0, chunks, start_keys, 0)
    for copy in loads[2:4]:
        copy.wait()
    lax.fori_loop(0, chunks, start_queries, 0)

    for d in far:
        @pl.when(me - d < 0)
        def _():
            kvb[d] = jnp.zeros(kvb.shape[1:], kvb.dtype)
            kseg[d] = jnp.full(kseg.shape[1:], -1, kseg.dtype)

        @pl.when(me + d >= count)
        def _():
            qgb[d] = jnp.zeros(qgb.shape[1:], qgb.dtype)
            qseg[d] = jnp.full(qseg.shape[1:], -1, qseg.dtype)
            stat[d] = jnp.zeros(stat.shape[1:], stat.dtype)

    own_col = jnp.broadcast_to(seg_row[0:1, :], (rows, rows)).T
    upper = lax.broadcasted_iota(jnp.int32, (rows, rows), 0)
    across = lax.broadcasted_iota(jnp.int32, (rows, rows), 1)
    same = own_col == seg_row[0:1, :]
    bias[0] = jnp.where(same & (across <= upper), 0.0, HIDDEN)
    bias_t[0] = jnp.where(same & (upper <= across), 0.0, HIDDEN)
    wait_many(lambda n: kseg.at[pl.ds(1, n)], seg_recv.at[0], me)
    wait_many(lambda n: qseg.at[pl.ds(1, n)], seg_recv.at[1], count - 1 - me)
    for d in far:
        bias[d] = jnp.where(own_col == kseg[d, 0:1, :], 0.0, HIDDEN)
        bias_t[d] = jnp.where(own_col == qseg[d, 0:1, :], 0.0, HIDDEN)
    step_y(0)

    first_lane = lax.broadcasted_iota(jnp.int32, (rows, head_dim), 1) == 0
    span = range(REACH + 1)

    def own_queries(c):
        cols = columns(c)
        query = load(2, 0, cols)
        grad = load(3, 0, cols)
        scores = [dot(query, load(0, d, cols), NT) * log2_scale + bias[d] for d in span]
        peak = jnp.max(functools.reduce(jnp.maximum, scores), -1, keepdims=True)
        exponent = [jnp.exp2(s - peak) for s in scores]
        total = jnp.sum(functools.reduce(jnp.add, exponent), -1, keepdims=True)
        inverse = 1.0 / total
        weights = [(e * inverse).astype(jnp.bfloat16) for e in exponent]
        attended = functools.reduce(
            jnp.add, [dot(weights[d], load(1, d, cols), NN) for d in span]
        ).astype(jnp.bfloat16)
        o_out[:, cols] = attended
        delta = jnp.sum(grad.astype(jnp.float32) * attended.astype(jnp.float32), -1, keepdims=True)
        pair = jnp.where(first_lane, peak + jnp.log2(total), delta)
        stat[0, c] = pair.T[0:2]
        total_grad = None
        for d in span:
            dprob = dot(grad, load(1, d, cols), NT)
            dscore = (weights[d].astype(jnp.float32) * (dprob - delta)).astype(jnp.bfloat16)
            term = dot(dscore, load(0, d, cols), NN)
            total_grad = term if total_grad is None else total_grad + term
        dq_out[:, cols] = (total_grad * inv_root).astype(jnp.bfloat16)

    def own_keys(c):
        cols = columns(c)
        key = load(0, 0, cols)
        value = load(1, 0, cols)
        key_grad = value_grad = None
        for d in span:
            query = load(2, d, cols)
            grad = load(3, d, cols)
            lse = stat[d, c, 0:1, :]
            delta = stat[d, c, 1:2, :]
            scores = dot(key, query, NT) * log2_scale + bias_t[d]
            weights = jnp.exp2(scores - lse)
            dprob = dot(value, grad, NT)
            dscore = (weights * (dprob - delta)).astype(jnp.bfloat16)
            value_term = dot(weights.astype(jnp.bfloat16), grad, NN)
            key_term = dot(dscore, query, NN)
            value_grad = value_term if value_grad is None else value_grad + value_term
            key_grad = key_term if key_grad is None else key_grad + key_term
        dk_out[:, cols] = (key_grad * inv_root).astype(jnp.bfloat16)
        dv_out[:, cols] = value_grad.astype(jnp.bfloat16)

    def send_stats(c):
        for d in far:
            @pl.when(me - d >= 0)
            def _():
                pltpu.make_async_remote_copy(
                    src_ref=stat.at[0, c],
                    dst_ref=stat.at[d, c],
                    send_sem=stat_send.at[d - 1],
                    recv_sem=stat_recv.at[c],
                    device_id=to(me - d),
                    device_id_type=MESH,
                ).start()

    def arrive_queries(c):
        @pl.when(me - 1 >= 0)
        def _():
            landed(KV, 1, c)

        @pl.when((me - 3 >= 0) & jnp.logical_not((odd == 0) & active(KV, 4, c)))
        def _():
            landed(KV, 3, c)

    def arrive_keys(c):
        @pl.when(me + 1 < count)
        def _():
            landed(QG, 1, c)

        @pl.when((me + 3 < count) & jnp.logical_not((odd == 1) & active(QG, 4, c)))
        def _():
            landed(QG, 3, c)
        wait_many(lambda n: stat.at[pl.ds(1, n), c], stat_recv.at[c], count - 1 - me)

    def own_rest(c, carry):
        own_y(QG, c)
        return carry

    def query_step(c, carry):
        @pl.when(c + 1 < chunks)
        def _():
            step_y(c + 1)

        far_end(QG, c)

        @pl.when(c + 2 == chunks)
        def _():
            lax.fori_loop(FILL, chunks, own_rest, 0)

        arrive_queries(c)
        own_queries(c)
        send_stats(c)
        return carry

    def finish(c):
        for ts in (KV, QG):
            own = active(ts, 3, c) | active(ts, 5, c) | active(ts, 6, c)
            passed = active(ts, 4, c)
            for slots, there in ((2, own & passed), (1, own != passed)):
                @pl.when(there)
                def _():
                    part = bufs[ts].at[pl.ds(0, slots), :, :, columns(c)]
                    pltpu.make_async_copy(part, part, send_sem.at[ts, c]).wait()

    def finish_rest(c, carry):
        finish(c)
        return carry

    def key_step(c, carry):
        @pl.when(c + 1 < chunks)
        def _():
            near_end(QG, c + 1)
            relay(QG, c + 1)

        @pl.when(c >= LAG)
        def _():
            finish(c - LAG)

        arrive_keys(c)
        own_keys(c)
        return carry

    lax.fori_loop(0, chunks, query_step, 0)
    near_end(QG, 0)
    relay(QG, 0)
    lax.fori_loop(0, chunks, key_step, 0)

    lax.fori_loop(chunks - LAG, chunks, finish_rest, 0)
    for ts in (KV, QG):
        for kind in range(3):
            @pl.when(active(ts, kind, 0))
            def _():
                pltpu.make_async_copy(bufs[ts].at[0], bufs[ts].at[0], whole_sem.at[ts, kind]).wait()
    for d in far:
        @pl.when(me - d >= 0)
        def _():
            pltpu.make_async_copy(stat.at[0], stat.at[0], stat_send.at[d - 1]).wait()

    wait_many(lambda n: kseg.at[pl.ds(1, n)], seg_send.at[0], count - 1 - me)
    wait_many(lambda n: kseg.at[pl.ds(1, n)], seg_send.at[1], me)


def drain(*refs):
    ins, outs, sem = refs[:4], refs[4:8], refs[8]
    copies = [pltpu.make_async_copy(ins[t], outs[t], sem.at[t]) for t in range(4)]
    for copy in copies:
        copy.start()
    for copy in copies:
        copy.wait()


def solution(mesh):
    count = mesh.shape["seq"]

    def local(queries, keys, values, out_grad, segments):
        rows, feature = queries.shape
        head_dim = feature // HEADS
        vmem = pl.BlockSpec(memory_space=pltpu.VMEM)
        slots = REACH + 1
        block = pltpu.VMEM((slots + 1, 2, rows, feature), queries.dtype)
        seg_block = pltpu.VMEM((slots, 1, rows), jnp.int32)
        mask = pltpu.VMEM((slots, rows, rows), jnp.float32)
        dma = pltpu.SemaphoreType.DMA
        shapes = [jax.ShapeDtypeStruct((rows, feature), jnp.bfloat16)] * 4
        results = pl.pallas_call(
            functools.partial(kernel, count, rows, head_dim),
            out_shape=shapes,
            in_specs=[pl.BlockSpec(memory_space=pl.ANY)] * 5,
            out_specs=[vmem] * 4,
            scratch_shapes=[block] * 2 + [
                pltpu.VMEM((1, rows), jnp.int32), seg_block, seg_block,
                pltpu.VMEM((slots, HEADS, 2, rows), jnp.float32),
                mask, mask,
                dma((5,)), dma((2, 3)), dma((2, HEADS)), dma((2, slots, HEADS)),
                dma((2,)), dma((2,)), dma((REACH,)), dma((HEADS,)),
            ],
            compiler_params=pltpu.CompilerParams(
                collective_id=0, has_side_effects=True, vmem_limit_bytes=VMEM_LIMIT
            ),
        )(queries, keys, values, out_grad, segments[None, :])
        return pl.pallas_call(
            drain,
            out_shape=shapes,
            in_specs=[vmem] * 4,
            out_specs=[pl.BlockSpec(memory_space=pl.ANY)] * 4,
            scratch_shapes=[dma((4,))],
            compiler_params=pltpu.CompilerParams(vmem_limit_bytes=DRAIN_LIMIT),
        )(*results)

    rows_spec = P(("branch", "seq"), None)
    return jax.shard_map(
        local,
        mesh=mesh,
        in_specs=(rows_spec,) * 4 + (P(("branch", "seq")),),
        out_specs=(rows_spec,) * 4,
        check_vma=False,
    )
```
